32 devices in a mesh: node: 16 (over z, y, x), hand: 2 (over core).
Axes of the slice: x: 2, y: 2, z: 4, core: 2. Of those that a mesh axis runs over, the one named last changes fastest.
Arguments:
- ranges: bfloat16 [512, 128, 1326], P('node', None, 'hand'), may hold values from 0.00019931793 to 0.0039978027
- strengths: int32 [512, 1326], P('node'), may hold values from 0 to 399
- live_hands: int32 [512, 1326], P('node'), may hold values 0 or 1
- pot_sizes: float32 [512, 128], P('node'), may hold values from 1 to 16
- action_counts: int32 [512], P('node'), may hold values from 1 to 8
- parents: int32 [512], P('node'), may hold values from 0 to 63
- turn_counts: int32 [16], replicated, may hold values from 1 to 4
- root_reach: float32 [16, 2, 1326], P(None, None, 'hand'), may hold values from 0.01 to 1
Outputs:
- turn_values: float32 [16, 2, 1326], P('node', None, 'hand')
- exploitability: float32 [], replicated
The draws below stay inside these ranges and needn't reach their ends.
All inputs are finite; a program needn't handle non-finite values. No bound on the sum of `live_hands` on one device may be relied on, other than what follows from the above.
Results may differ from the reference program's by a relative error of at most 0.0003.
Values may be sent and summed in bfloat16 or wider, within the bound.
A program may use at most 128 MiB of HBM per device.

```python
import math
import jax
import jax.numpy as jnp
import numpy as np
from jax import lax

H = 1326
ACT = 8
GROUPS = 8
TACT = 4
LINES = 64
NODES = 512
TURNS = 16


def with_ends(values, rng, low, high):
    longest = values.shape.index(max(values.shape))
    spots = []
    for shift in (0, 1):
        where = [jax.random.randint(jax.random.fold_in(rng, axis), (), 0, length) for axis, length in enumerate(values.shape)]
        where[longest] = (where[longest] + shift) % values.shape[longest]
        spots.append(tuple(where))
    return values.at[spots[0]].set(low).at[spots[1]].set(high)


def block_scale(rng, extent, cuts, low, top_value):
    factor_of = 1.0
    for dim, blocks in cuts:
        steps = jax.random.uniform(jax.random.fold_in(jax.random.fold_in(rng, 6), dim), (blocks,), jnp.float32, low / len(cuts), top_value / len(cuts))
        factor_of = factor_of * jnp.repeat(jnp.exp(steps), extent[dim] // blocks).reshape((-1,) + (1,) * (len(extent) - 1 - dim))
    return factor_of


def setup_inputs(seed: int = 0) -> dict:
    key_of = jax.random.split(jax.random.key(seed), 9)
    ranges = jnp.clip(jnp.exp(math.log(0.0039978027) - 2.998599 * jax.random.uniform(key_of[0], (NODES, 2 * LINES, H), jnp.float32) ** block_scale(key_of[0], (NODES, 2 * LINES, H), ((0, 16), (2, 2)), -0.2, 0.2)), 0.00019931793, 0.0039978027).astype(jnp.bfloat16)
    strengths = with_ends(jax.random.randint(key_of[1], (NODES, H), 0, 400), jax.random.fold_in(key_of[1], 1), 0, 399).astype(jnp.int32)
    live_hands = with_ends((jax.random.randint(key_of[2], (NODES, H), 0, 10) < 9).astype(jnp.int32), jax.random.fold_in(key_of[2], 1), 0, 1)
    pot_sizes = jnp.clip(jnp.exp(math.log(16.0) - 2.7725887 * jax.random.uniform(key_of[3], (NODES, 2 * LINES), jnp.float32) ** block_scale(key_of[3], (NODES, 2 * LINES), ((0, 16),), -0.2, 0.2)), 1.0, 16.0)
    action_counts = with_ends(jax.random.randint(key_of[4], (NODES,), 1, ACT + 1), jax.random.fold_in(key_of[4], 1), 1, ACT).astype(jnp.int32)
    parents = with_ends(jax.random.randint(key_of[5], (NODES,), 0, TURNS * TACT), jax.random.fold_in(key_of[5], 1), 0, (TURNS * TACT) - 1).astype(jnp.int32)
    turn_counts = with_ends(jax.random.randint(key_of[6], (TURNS,), 1, TACT + 1), jax.random.fold_in(key_of[6], 1), 1, TACT).astype(jnp.int32)
    root_reach = jnp.clip(jnp.exp(math.log(1.0) - 4.6051702 * jax.random.uniform(key_of[7], (TURNS, 2, H), jnp.float32) ** block_scale(key_of[7], (TURNS, 2, H), ((2, 2),), -0.2, 0.2)), 0.01, 1.0)
    return dict(ranges=ranges, strengths=strengths, live_hands=live_hands, pot_sizes=pot_sizes, action_counts=action_counts, parents=parents, turn_counts=turn_counts, root_reach=root_reach)


def card_pairs(wanted):
    first_list = []
    second_list = []
    for lower_card in range(52):
        for upper_card in range(lower_card + 1, 52):
            first_list.append(lower_card)
            second_list.append(upper_card)
    return (jnp.asarray(np.array(first_list[:wanted], dtype=np.int32)),
            jnp.asarray(np.array(second_list[:wanted], dtype=np.int32)))


def pair_compat(row_first, row_second, col_first, col_second):
    shared = (row_first[:, None] == col_first[None, :]) | (row_first[:, None] == col_second[None, :])
    shared = shared | (row_second[:, None] == col_first[None, :]) | (row_second[:, None] == col_second[None, :])
    return jnp.where(shared, 0.0, 1.0).astype(jnp.float32)


def reference(ranges, strengths, live_hands, pot_sizes, action_counts, parents, turn_counts, root_reach):
    first_card, second_card = card_pairs(H)
    compat = pair_compat(first_card, second_card, first_card, second_card)

    def node_best(packed):
        strength, live_row, reach_rows, pot_row, legal = packed
        live_float = live_row.astype(jnp.float32)
        signs = jnp.sign((strength[:, None] - strength[None, :]).astype(jnp.float32))
        matrix = signs * compat * live_float[:, None] * live_float[None, :]
        values = jnp.dot(reach_rows.astype(jnp.float32), matrix.T, precision=lax.Precision.HIGHEST)
        values = (values * pot_row[:, None]).reshape(2, GROUPS, ACT, H)
        usable = jnp.arange(ACT) < legal
        best = jnp.where(usable[None, None, :, None], values, -1e30).max(axis=2)
        return jnp.sum(best, axis=1)

    river_best = lax.map(node_best, (strengths, live_hands, ranges, pot_sizes, action_counts))
    sums = jax.ops.segment_sum(river_best, parents, num_segments=TURNS * TACT)
    sums = sums.reshape(TURNS, TACT, 2, H)
    usable = jnp.arange(TACT)[None, :] < turn_counts[:, None]
    turn_values = jnp.where(usable[:, :, None, None], sums, -1e30).max(axis=1)
    exploitability = jnp.sum(root_reach * turn_values)
    return turn_values, exploitability
```

```python
import functools

import jax
import jax.numpy as jnp
import numpy as np
from jax import lax
from jax.experimental import pallas as pl
from jax.experimental.pallas import tpu as pltpu
from jax.sharding import PartitionSpec as P

ACT = 8
GROUPS = 8
TACT = 4
LANE = 128
PACK = 16
WIDE = 256
TALL = 8
PAIR = 4
MESH = pl.DeviceIdType.MESH
MID = 200.0
LOW = -1e30


def card_rows(hands, half, tiles):
    pairs = [(a, b) for a in range(52) for b in range(a + 1, 52)][:hands]
    flat = np.array(pairs, np.float32).T
    rows = np.zeros((2, 8, tiles * LANE), np.float32)
    for side in range(2):
        rows[side, :2, :half] = flat[:, side * half : (side + 1) * half]
    return jnp.asarray(rows.reshape(2, 8, tiles, LANE).transpose(0, 2, 1, 3))


def kernel(
    sizes,
    ranges,
    strengths,
    live,
    pots,
    legal,
    parents,
    turn_legal,
    reach,
    cards,
    best_out,
    total_out,
    raw,
    loose,
    lines,
    row_s,
    row_live,
    col_s,
    wide,
    compat,
    pot_wide,
    values,
    river,
    river_in,
    chosen,
    part,
    got_plane,
    mid,
    got_line,
    shares,
    line_shares,
    local_sem,
    send_sem,
    recv_sem,
    river_send,
    river_recv,
    plane_send,
    plane_recv,
    line_send,
    line_recv,
    tell_send,
    tell_recv,
    tell2_send,
    tell2_recv,
):
    n_node, low, high, nodes, half, tiles, turns_mine, rows_all = sizes
    f32, bf16 = jnp.float32, jnp.bfloat16
    node = lax.axis_index("node")
    hand = lax.axis_index("hand")
    q = lax.rem(node, low)
    z = node // low
    mine = nodes // 2
    spans = mine // TALL
    blocks = tiles // 2
    rows_k = tiles * LANE
    used = -(-half // PACK) * PACK
    first_row = pl.multiple_of(hand * mine, TALL)
    line_rows = 2 * GROUPS * ACT
    out_rows = turns_mine * 2 * TACT

    barrier = pltpu.get_barrier_semaphore()

    def plane_device(offset):
        spot = lax.rem(q * 2 + hand + offset, 2 * low)
        return spot, (z * low + spot // 2, lax.rem(spot, 2))

    def line_device(offset):
        spot = lax.rem(z + offset, high)
        return spot, (spot * low + q, hand)

    for offset in range(1, 2 * low):
        pl.semaphore_signal(
            barrier, inc=1, device_id=plane_device(offset)[1], device_id_type=MESH
        )
    for offset in range(1, high):
        pl.semaphore_signal(
            barrier, inc=1, device_id=line_device(offset)[1], device_id_type=MESH
        )

    def local_copy(span):
        at = pl.multiple_of(hand * mine + span * TALL, TALL)
        return pltpu.make_async_copy(
            ranges.at[:, pl.ds(at, TALL), :],
            raw.at[hand, span, pl.ds(0, half)],
            local_sem.at[span],
        )

    def peer_copy(span):
        at = pl.multiple_of((1 - hand) * mine + span * TALL, TALL)
        return pltpu.make_async_remote_copy(
            src_ref=ranges.at[:, pl.ds(at, TALL), :],
            dst_ref=raw.at[hand, span, pl.ds(0, half)],
            send_sem=send_sem.at[span],
            recv_sem=recv_sem.at[span],
            device_id=(node, 1 - hand),
            device_id_type=MESH,
        )

    for span in range(spans):
        local_copy(span).start()

    for side in range(2):
        for span in range(spans):
            raw[side, span, half:] = jnp.zeros((rows_k - half, TALL, LANE), bf16)

    row_s[...] = jnp.zeros_like(row_s)
    row_live[...] = jnp.zeros_like(row_live)
    strength = strengths[pl.ds(first_row, mine), :].astype(f32) - MID
    alive = live[pl.ds(first_row, mine), :].astype(f32)
    for side in range(2):
        for tile in range(tiles):
            width = min(LANE, half - tile * LANE)
            cut = slice(side * half + tile * LANE, side * half + tile * LANE + width)
            row_s[side, tile, :mine, :width] = strength[:, cut]
            row_live[side, tile, :, :width] = alive[:, cut]
            row_s[side, tile, mine : mine + 8, :] = cards[side, tile]

    pl.semaphore_wait(barrier, 2 * low - 1 + high - 1)
    for span in range(spans):
        peer_copy(span).start()

    def turn_rows(tile, carry):
        for side in range(2):
            col_s[side * tiles + tile] = row_s[side, tile].T
        return carry

    lax.fori_loop(0, tiles, turn_rows, 0)

    def compat_rows(tile, carry):
        column = col_s[tile]
        at = pl.ds(pl.multiple_of(tile * LANE, LANE), LANE)
        first = jnp.broadcast_to(column[:, mine : mine + 1], (LANE, LANE)).astype(bf16)
        second = jnp.broadcast_to(column[:, mine + 1 : mine + 2], (LANE, LANE)).astype(bf16)
        one = jnp.ones((LANE, LANE), bf16)
        zero = jnp.zeros((LANE, LANE), bf16)
        for side in range(2):
            for spot in range(tiles):
                a = jnp.broadcast_to(row_s[side, spot, mine : mine + 1, :], (LANE, LANE)).astype(bf16)
                b = jnp.broadcast_to(row_s[side, spot, mine + 1 : mine + 2, :], (LANE, LANE)).astype(bf16)
                shared = (first == a) | (first == b) | (second == a) | (second == b)
                compat[side * tiles + spot, at, :] = jnp.where(shared, zero, one)
        for n in range(mine):
            spread = jnp.broadcast_to(column[:, n : n + 1], (LANE, LANE))
            wide[n, at, :] = spread.astype(bf16)
        return carry

    lax.fori_loop(0, 2 * tiles, compat_rows, 0)

    pot_block = jnp.concatenate(
        [pots[pl.ds(first_row, mine), :], jnp.zeros((LANE - mine, line_rows), f32)], axis=0
    ).T
    for n in range(mine):
        pot_wide[n] = jnp.broadcast_to(pot_block[:, n : n + 1], (line_rows, LANE))

    group = 2 * mine
    depth = 2 * 3 * group
    source = lax.broadcasted_iota(jnp.int32, (group, depth), 0)
    column_at = lax.broadcasted_iota(jnp.int32, (group, depth), 1)
    owner = lax.rem(lax.rem(column_at, group) + hand * mine, group)
    pick = jnp.where(source == owner, 1.0, 0.0).astype(bf16)
    parent_rows = jnp.broadcast_to(parents[...].astype(f32), (16, nodes)).astype(bf16)
    parent_of = jnp.dot(parent_rows, pick, preferred_element_type=f32)[:1]
    row_at = lax.broadcasted_iota(jnp.int32, (rows_all, depth), 0)
    depth_at = lax.broadcasted_iota(jnp.int32, (rows_all, depth), 1)
    wanted = (row_at // (2 * TACT)) * TACT + lax.rem(row_at, TACT)
    same = lax.rem(row_at // TACT, 2) == depth_at // (3 * group)
    match = jnp.broadcast_to(parent_of, (rows_all, depth)) == wanted.astype(f32)
    chosen[...] = jnp.where(match & same, 1.0, 0.0).astype(bf16)

    def spread_lines(side, span):
        def one_tile(tile, carry):
            at = pl.ds(pl.multiple_of(tile * LANE, LANE), LANE)
            loose[...] = raw[side, span, at].astype(f32).reshape(LANE * TALL, LANE)
            for u in range(TALL):
                n = span * TALL + u
                block = loose[pl.ds(u, LANE, stride=TALL), :].astype(bf16).T
                keep = row_live[side, tile, pl.ds(n, 1), :].astype(bf16)
                lines[n, side * tiles + tile] = block * keep
            return carry

        lax.fori_loop(0, tiles, one_tile, 0)

    for span in range(spans):
        local_copy(span).wait()
        spread_lines(hand, span)

    def river_copy(b):
        return pltpu.make_async_remote_copy(
            src_ref=river.at[1 - hand, b],
            dst_ref=river_in.at[b],
            send_sem=river_send.at[b],
            recv_sem=river_recv.at[b],
            device_id=(node, 1 - hand),
            device_id_type=MESH,
        )

    def plane_copy(b, offset):
        spot = lax.rem(q + offset, low)
        return pltpu.make_async_remote_copy(
            src_ref=part.at[b, spot],
            dst_ref=got_plane.at[b, offset - 1],
            send_sem=plane_send.at[b, offset - 1],
            recv_sem=plane_recv.at[b, offset - 1],
            device_id=(z * low + spot, hand),
            device_id_type=MESH,
        )

    def line_copy(b, offset):
        spot, device = line_device(offset)
        return pltpu.make_async_remote_copy(
            src_ref=mid.at[b, spot],
            dst_ref=got_line.at[b, offset - 1],
            send_sem=line_send.at[b, offset - 1],
            recv_sem=line_recv.at[b, offset - 1],
            device_id=device,
            device_id_type=MESH,
        )

    def sum_block(b):
        river_copy(b).wait_recv()
        pieces = []
        for player in range(2):
            rest = jnp.concatenate(
                [
                    jnp.concatenate([river[hand, b, player, j], river_in[b, player, j]], axis=0)
                    for j in range(2)
                ],
                axis=1,
            )
            for _ in range(3):
                piece = rest.astype(bf16)
                pieces.append(piece)
                rest = rest - piece.astype(f32)
        sums = jnp.dot(
            chosen[...], jnp.concatenate(pieces, axis=0), preferred_element_type=f32
        )
        for other in range(n_node):
            part[b, other % low, other // low] = sums[other * out_rows : (other + 1) * out_rows]
        for offset in range(1, low):
            plane_copy(b, offset).start()

    def pass_block(b):
        whole = part[b, q]
        for offset in range(1, low):
            plane_copy(b, offset).wait_recv()
            whole = whole + got_plane[b, offset - 1]
        mid[b] = whole
        for offset in range(1, high):
            line_copy(b, offset).start()

    steps = mine // PAIR

    def one_step(step, carry):
        b = step // steps
        p = lax.rem(step, steps)
        for span in range(spans):

            @pl.when(step == span * TALL // PAIR)
            def _():
                peer_copy(span).wait_recv()
                spread_lines(1 - hand, span)

        for u in range(PAIR):
            n = p * PAIR + u
            left = jnp.concatenate([lines[n, k] for k in range(2 * tiles)], axis=1)
            columns = []
            for side in range(2):
                for j in range(2):
                    hero = row_s[side, 2 * b + j, pl.ds(n, 1), :]
                    hero = jnp.broadcast_to(hero, (PACK, LANE)).astype(bf16)
                    hero = jnp.concatenate([hero] * (used // PACK), axis=0)
                    stack = []
                    for other in range(2):
                        at = slice(other * rows_k, other * rows_k + used)
                        upper = compat[side * tiles + 2 * b + j, at, :]
                        gap = hero - wide[n, at, :]
                        stack.append(lax.clamp(jnp.bfloat16(-1), gap * upper, jnp.bfloat16(1)))
                        if rows_k > used:
                            stack.append(jnp.zeros((rows_k - used, LANE), bf16))
                    columns.append(jnp.concatenate(stack, axis=0))
            signs = jnp.concatenate(columns, axis=1)
            result = jnp.dot(left, signs, preferred_element_type=f32)
            last = jnp.maximum(legal[hand * mine + n] - 1, 0)
            for side in range(2):
                for j in range(2):
                    spot = side * 2 + j
                    values[u, spot] = result[:, spot * LANE : (spot + 1) * LANE] * pot_wide[n]
                    best = values[u, spot, pl.ds(0, 2 * GROUPS, stride=ACT), :]
                    for a in range(1, ACT):
                        row = jnp.minimum(last, a)
                        best = jnp.maximum(
                            best, values[u, spot, pl.ds(row, 2 * GROUPS, stride=ACT), :]
                        )
                    keep = row_live[side, 2 * b + j, pl.ds(n, 1), :]
                    for player in range(2):
                        total = jnp.sum(
                            best[player * GROUPS : (player + 1) * GROUPS], axis=0, keepdims=True
                        )
                        river[side, b, player, j, pl.ds(n, 1), :] = total * keep

        @pl.when(p == steps - 1)
        def _():
            river_copy(b).start()

        @pl.when((p == 0) & (b > 0))
        def _():
            sum_block(b - 1)

        @pl.when((p == steps // 2) & (b > 0))
        def _():
            pass_block(b - 1)

        return carry

    lax.fori_loop(0, blocks * steps, one_step, 0)
    sum_block(blocks - 1)
    pass_block(blocks - 1)

    columns = []
    for b in range(blocks):
        whole = mid[b, z]
        for offset in range(1, high):
            line_copy(b, offset).wait_recv()
            whole = whole + got_line[b, offset - 1]
        columns.append(whole)
    total = jnp.concatenate(columns, axis=1)

    kind = lax.rem(lax.broadcasted_iota(jnp.int32, (2 * TACT, rows_k), 0), TACT)
    share = jnp.zeros((1, half), f32)
    for t in range(turns_mine):
        turn = node * turns_mine + t
        rows = total[t * 2 * TACT : (t + 1) * 2 * TACT]
        rows = jnp.where(kind < turn_legal[turn], rows, LOW)
        for player in range(2):
            best = jnp.max(rows[player * TACT : (player + 1) * TACT], axis=0, keepdims=True)
            best = best[:, :half]
            best_out[t, player : player + 1, :] = best
            share = share + reach[turn, player : player + 1, :] * best
    me = q * 2 + hand
    shares[me] = jnp.broadcast_to(jnp.sum(share, axis=1, keepdims=True), (8, LANE))

    def tell_plane(offset, back):
        to, device = plane_device(offset)
        source = lax.rem(me + 2 * low - offset, 2 * low) if back else me
        return pltpu.make_async_remote_copy(
            src_ref=shares.at[me],
            dst_ref=shares.at[source],
            send_sem=tell_send.at[offset - 1],
            recv_sem=tell_recv.at[offset - 1],
            device_id=device,
            device_id_type=MESH,
        )

    def tell_line(offset, back):
        to, device = line_device(offset)
        source = lax.rem(z + high - offset, high) if back else z
        return pltpu.make_async_remote_copy(
            src_ref=line_shares.at[z],
            dst_ref=line_shares.at[source],
            send_sem=tell2_send.at[offset - 1],
            recv_sem=tell2_recv.at[offset - 1],
            device_id=device,
            device_id_type=MESH,
        )

    for offset in range(1, 2 * low):
        tell_plane(offset, False).start()
    for offset in range(1, 2 * low):
        tell_plane(offset, True).wait_recv()
    whole = shares[0]
    for spot in range(1, 2 * low):
        whole = whole + shares[spot]
    line_shares[z] = whole
    for offset in range(1, high):
        tell_line(offset, False).start()
    for offset in range(1, high):
        tell_line(offset, True).wait_recv()
    whole = line_shares[0]
    for spot in range(1, high):
        whole = whole + line_shares[spot]
    total_out[0, 0] = whole[0, 0]

    for span in range(spans):
        peer_copy(span).wait_send()
    for b in range(blocks):
        river_copy(b).wait_send()
        for offset in range(1, low):
            plane_copy(b, offset).wait_send()
        for offset in range(1, high):
            line_copy(b, offset).wait_send()
    for offset in range(1, 2 * low):
        tell_plane(offset, False).wait_send()
    for offset in range(1, high):
        tell_line(offset, False).wait_send()


def solution(mesh):
    n_node = mesh.shape["node"]
    high = min(4, n_node)
    low = n_node // high

    def local(
        ranges, strengths, live_hands, pot_sizes, action_counts, parents, turn_counts, root_reach
    ):
        nodes, line_rows, half = ranges.shape
        hands = strengths.shape[1]
        tiles = -(-half // WIDE) * 2
        blocks = tiles // 2
        turns_all = turn_counts.shape[0]
        turns_mine = turns_all // n_node
        rows_all = turns_all * 2 * TACT
        out_rows = turns_mine * 2 * TACT
        mine = nodes // 2
        spans = mine // TALL
        f32, bf16 = jnp.float32, jnp.bfloat16
        vmem = pl.BlockSpec(memory_space=pltpu.VMEM)
        smem = pl.BlockSpec(memory_space=pltpu.SMEM)
        hbm = pl.BlockSpec(memory_space=pl.ANY)
        dma = pltpu.SemaphoreType.DMA
        sizes = (n_node, low, high, nodes, half, tiles, turns_mine, rows_all)
        best, total = pl.pallas_call(
            functools.partial(kernel, sizes),
            out_shape=(
                jax.ShapeDtypeStruct((turns_mine, 2, half), f32),
                jax.ShapeDtypeStruct((1, 1), f32),
            ),
            in_specs=[hbm, vmem, vmem, vmem, smem, vmem, smem, vmem, vmem],
            out_specs=(vmem, smem),
            scratch_shapes=[
                pltpu.VMEM((2, spans, tiles * LANE, TALL, line_rows), bf16),
                pltpu.VMEM((LANE * TALL, line_rows), f32),
                pltpu.VMEM((mine, 2 * tiles, line_rows, LANE), bf16),
                pltpu.VMEM((2, tiles, LANE, LANE), f32),
                pltpu.VMEM((2, tiles, mine, LANE), f32),
                pltpu.VMEM((2 * tiles, LANE, LANE), f32),
                pltpu.VMEM((mine, 2 * tiles * LANE, LANE), bf16),
                pltpu.VMEM((2 * tiles, 2 * tiles * LANE, LANE), bf16),
                pltpu.VMEM((mine, line_rows, LANE), f32),
                pltpu.VMEM((PAIR, 4, line_rows, LANE), f32),
                pltpu.VMEM((2, blocks, 2, 2, mine, LANE), f32),
                pltpu.VMEM((blocks, 2, 2, mine, LANE), f32),
                pltpu.VMEM((rows_all, 12 * mine), bf16),
                pltpu.VMEM((blocks, low, high, out_rows, WIDE), f32),
                pltpu.VMEM((blocks, low - 1, high, out_rows, WIDE), f32),
                pltpu.VMEM((blocks, high, out_rows, WIDE), f32),
                pltpu.VMEM((blocks, high - 1, out_rows, WIDE), f32),
                pltpu.VMEM((2 * low, 8, LANE), f32),
                pltpu.VMEM((high, 8, LANE), f32),
                dma((spans,)),
                dma((spans,)),
                dma((spans,)),
                dma((blocks,)),
                dma((blocks,)),
                dma((blocks, low - 1)),
                dma((blocks, low - 1)),
                dma((blocks, high - 1)),
                dma((blocks, high - 1)),
                dma((2 * low - 1,)),
                dma((2 * low - 1,)),
                dma((high - 1,)),
                dma((high - 1,)),
            ],
            compiler_params=pltpu.CompilerParams(
                collective_id=0, has_side_effects=True, vmem_limit_bytes=60 * 1024 * 1024
            ),
        )(
            jnp.transpose(ranges, (2, 0, 1)),
            strengths,
            live_hands,
            pot_sizes,
            action_counts,
            parents.reshape(1, nodes),
            turn_counts,
            root_reach,
            card_rows(hands, half, tiles),
        )
        return best, total.reshape(())

    in_specs = (
        P("node", None, "hand"),
        P("node", None),
        P("node", None),
        P("node", None),
        P("node"),
        P("node"),
        P(),
        P(None, None, "hand"),
    )
    out_specs = (P("node", None, "hand"), P())
    return jax.shard_map(local, mesh=mesh, in_specs=in_specs, out_specs=out_specs, check_vma=False)
```

```python
import functools

import jax
import jax.numpy as jnp
import numpy as np
from jax import lax
from jax.experimental import pallas as pl
from jax.experimental.pallas import tpu as pltpu
from jax.sharding import PartitionSpec as P

ACT = 8
GROUPS = 8
TACT = 4
LANE = 128
PACK = 16
WIDE = 256
TALL = 8
PAIR = 4
MESH = pl.DeviceIdType.MESH
MID = 200.0
LOW = -1e30


def compat_table(hands, half, tiles):
    pairs = [(a, b) for a in range(52) for b in range(a + 1, 52)][:hands]
    holds = np.zeros((hands, 52), np.int32)
    for hand, (a, b) in enumerate(pairs):
        holds[hand, a] = holds[hand, b] = 1
    apart = (holds @ holds.T) == 0
    table = np.zeros((2, tiles * LANE, 2, tiles * LANE), np.int8)
    table[:, :half, :, :half] = apart.reshape(2, half, 2, half)
    table = table.reshape(2 * tiles * LANE, 2 * tiles, LANE).transpose(1, 0, 2)
    return jnp.asarray(table)


def kernel(
    sizes,
    ranges,
    strengths,
    live,
    pots,
    legal,
    parents,
    turn_legal,
    reach,
    table,
    best_out,
    total_out,
    raw,
    loose,
    lines,
    row_s,
    row_live,
    col_s,
    wide,
    small,
    compat,
    pot_wide,
    turned,
    river,
    river_in,
    chosen,
    part,
    got_plane,
    got_line,
    found,
    shares,
    table_sem,
    local_sem,
    send_sem,
    recv_sem,
    river_send,
    river_recv,
    plane_send,
    plane_recv,
    line_send,
    line_recv,
    tell_send,
    tell_recv,
):
    n_node, low, high, nodes, half, tiles, turns_mine, rows_all = sizes
    f32, bf16 = jnp.float32, jnp.bfloat16
    node = lax.axis_index("node")
    hand = lax.axis_index("hand")
    q = lax.rem(node, low)
    z = node // low
    mine = nodes // 2
    spans = mine // TALL
    blocks = tiles // 2
    rows_k = tiles * LANE
    used = -(-half // PACK) * PACK
    first_row = pl.multiple_of(hand * mine, TALL)
    each = 2 * GROUPS
    line_rows = each * ACT
    out_rows = turns_mine * 2 * TACT

    barrier = pltpu.get_barrier_semaphore()

    def plane_device(offset):
        spot = lax.rem(q * 2 + hand + offset, 2 * low)
        return spot, (z * low + spot // 2, lax.rem(spot, 2))

    def line_device(offset):
        spot = lax.rem(z + offset, high)
        return spot, (spot * low + q, hand)

    for offset in range(1, 2 * low):
        pl.semaphore_signal(
            barrier, inc=1, device_id=plane_device(offset)[1], device_id_type=MESH
        )
    for offset in range(1, high):
        pl.semaphore_signal(
            barrier, inc=1, device_id=line_device(offset)[1], device_id_type=MESH
        )

    def local_copy(span):
        at = pl.multiple_of(hand * mine + span * TALL, TALL)
        return pltpu.make_async_copy(
            ranges.at[:, pl.ds(at, TALL), :],
            raw.at[hand, span, pl.ds(0, half)],
            local_sem.at[span],
        )

    def peer_copy(span):
        at = pl.multiple_of((1 - hand) * mine + span * TALL, TALL)
        return pltpu.make_async_remote_copy(
            src_ref=ranges.at[:, pl.ds(at, TALL), :],
            dst_ref=raw.at[hand, span, pl.ds(0, half)],
            send_sem=send_sem.at[span],
            recv_sem=recv_sem.at[span],
            device_id=(node, 1 - hand),
            device_id_type=MESH,
        )

    table_copy = pltpu.make_async_copy(table, small, table_sem)
    for span in range(spans):
        local_copy(span).start()
    table_copy.start()

    for side in range(2):
        for span in range(spans):
            raw[side, span, half:] = jnp.zeros((rows_k - half, TALL, LANE), bf16)

    row_s[...] = jnp.zeros_like(row_s)
    row_live[...] = jnp.zeros_like(row_live)
    strength = strengths[pl.ds(first_row, mine), :].astype(f32) - MID
    alive = live[pl.ds(first_row, mine), :].astype(f32)
    for side in range(2):
        for tile in range(tiles):
            width = min(LANE, half - tile * LANE)
            cut = slice(side * half + tile * LANE, side * half + tile * LANE + width)
            row_s[side, tile, :mine, :width] = strength[:, cut]
            row_live[side, tile, :, :width] = alive[:, cut]

    pl.semaphore_wait(barrier, 2 * low - 1 + high - 1)
    for span in range(spans):
        peer_copy(span).start()

    def turn_rows(tile, carry):
        for side in range(2):
            col_s[side * tiles + tile] = row_s[side, tile].T
        return carry

    lax.fori_loop(0, tiles, turn_rows, 0)

    table_copy.wait()

    def compat_rows(tile, carry):
        at = pl.ds(pl.multiple_of(tile * LANE, LANE), LANE)
        for spot in range(2 * tiles):
            compat[spot, at, :] = small[spot, at, :].astype(bf16)
        for n in range(mine):
            spread = jnp.broadcast_to(col_s[tile, :, n : n + 1], (LANE, LANE))
            wide[n, at, :] = spread.astype(bf16)
        return carry

    lax.fori_loop(0, 2 * tiles, compat_rows, 0)

    pot_block = jnp.concatenate(
        [pots[pl.ds(first_row, mine), :], jnp.zeros((LANE - mine, line_rows), f32)], axis=0
    ).T
    turned[0][...] = pot_block
    for a in range(ACT):
        rows = turned[0][pl.ds(a, each, stride=ACT), :]
        for n in range(mine):
            pot_wide[n, a * each : (a + 1) * each] = jnp.broadcast_to(rows[:, n : n + 1], (each, LANE))

    group = 2 * mine
    depth = 2 * 3 * group
    source = lax.broadcasted_iota(jnp.int32, (group, depth), 0)
    column_at = lax.broadcasted_iota(jnp.int32, (group, depth), 1)
    owner = lax.rem(lax.rem(column_at, group) + hand * mine, group)
    pick = jnp.where(source == owner, 1.0, 0.0).astype(bf16)
    parent_rows = jnp.broadcast_to(parents[...].astype(f32), (16, nodes)).astype(bf16)
    parent_of = jnp.dot(parent_rows, pick, preferred_element_type=f32)[:1]
    row_at = lax.broadcasted_iota(jnp.int32, (rows_all, depth), 0)
    depth_at = lax.broadcasted_iota(jnp.int32, (rows_all, depth), 1)
    wanted = (row_at // (2 * TACT)) * TACT + lax.rem(row_at, TACT)
    same = lax.rem(row_at // TACT, 2) == depth_at // (3 * group)
    match = jnp.broadcast_to(parent_of, (rows_all, depth)) == wanted.astype(f32)
    chosen[...] = jnp.where(match & same, 1.0, 0.0).astype(bf16)

    def spread_lines(side, span):
        for tile in range(tiles):
            width = min(LANE, -(-(half - tile * LANE) // PACK) * PACK)
            bank = tile % 2
            block = raw[side, span, tile * LANE : tile * LANE + width].astype(f32)
            loose[bank][: width * TALL] = block.reshape(width * TALL, LANE)
            for u in range(TALL):
                n = span * TALL + u
                turn = turned[bank * TALL + u]
                turn[:, :width] = loose[bank][pl.ds(u, width, stride=TALL), :].T
                keep = row_live[side, tile, pl.ds(n, 1), :width]
                for a in range(ACT):
                    rows = turn[pl.ds(a, each, stride=ACT), :][:, :width] * keep
                    at = slice(a * each, (a + 1) * each)
                    lines[n, side * tiles + tile, at, :width] = rows.astype(bf16)

    for n in range(mine):
        for side in range(2):
            lines[n, side * tiles + half // LANE] = jnp.zeros((line_rows, LANE), bf16)

    def own_span(span, carry):
        local_copy(span).wait()
        spread_lines(hand, span)
        return carry

    lax.fori_loop(0, spans, own_span, 0)

    def river_copy(b):
        return pltpu.make_async_remote_copy(
            src_ref=river.at[1 - hand, b],
            dst_ref=river_in.at[b],
            send_sem=river_send.at[b],
            recv_sem=river_recv.at[b],
            device_id=(node, 1 - hand),
            device_id_type=MESH,
        )

    def plane_copy(b, offset):
        spot = lax.rem(q + offset, low)
        return pltpu.make_async_remote_copy(
            src_ref=part.at[b, spot],
            dst_ref=got_plane.at[b, offset - 1],
            send_sem=plane_send.at[b, offset - 1],
            recv_sem=plane_recv.at[b, offset - 1],
            device_id=(z * low + spot, hand),
            device_id_type=MESH,
        )

    def line_copy(b, offset, back=False):
        spot, device = line_device(offset)
        source = lax.rem(z + high - offset, high) if back else z
        return pltpu.make_async_remote_copy(
            src_ref=got_line.at[b, z],
            dst_ref=got_line.at[b, source],
            send_sem=line_send.at[b, offset - 1],
            recv_sem=line_recv.at[b, offset - 1],
            device_id=device,
            device_id_type=MESH,
        )

    def sum_block(b):
        river_copy(b).wait_recv()
        pieces = []
        for player in range(2):
            rest = jnp.concatenate(
                [
                    jnp.concatenate([river[hand, b, player, j], river_in[b, player, j]], axis=0)
                    for j in range(2)
                ],
                axis=1,
            )
            for _ in range(3):
                piece = rest.astype(bf16)
                pieces.append(piece)
                rest = rest - piece.astype(f32)
        sums = jnp.dot(
            chosen[...], jnp.concatenate(pieces, axis=0), preferred_element_type=f32
        )
        for other in range(n_node):
            part[b, other % low, other // low] = sums[other * out_rows : (other + 1) * out_rows]
        for offset in range(1, low):
            plane_copy(b, offset).start()

    def pass_block(b):
        whole = part[b, q]
        for offset in range(1, low):
            plane_copy(b, offset).wait_recv()
            whole = whole + got_plane[b, offset - 1]
        got_line[b, z] = whole
        for offset in range(1, high):
            line_copy(b, offset).start()

    def one_step(b, p, carry):
        for u in range(PAIR):
            n = p * PAIR + u
            left = jnp.concatenate([lines[n, k] for k in range(2 * tiles)], axis=1)
            columns = []
            for side in range(2):
                for j in range(2):
                    hero = row_s[side, 2 * b + j, pl.ds(n, 1), :]
                    hero = jnp.broadcast_to(hero, (PACK, LANE)).astype(bf16)
                    hero = jnp.concatenate([hero] * (used // PACK), axis=0)
                    stack = []
                    for other in range(2):
                        at = slice(other * rows_k, other * rows_k + used)
                        upper = compat[side * tiles + 2 * b + j, at, :]
                        gap = hero - wide[n, at, :]
                        stack.append(lax.clamp(jnp.bfloat16(-1), gap * upper, jnp.bfloat16(1)))
                        if rows_k > used:
                            stack.append(jnp.zeros((rows_k - used, LANE), bf16))
                    columns.append(jnp.concatenate(stack, axis=0))
            signs = jnp.concatenate(columns, axis=1)
            result = jnp.dot(left, signs, preferred_element_type=f32)
            count = legal[hand * mine + n]
            for side in range(2):
                for j in range(2):
                    spot = side * 2 + j
                    rows = result[:, spot * LANE : (spot + 1) * LANE]
                    best = rows[:each] * pot_wide[n, :each]
                    for a in range(1, ACT):
                        at = slice(a * each, (a + 1) * each)
                        best = jnp.maximum(best, jnp.where(a < count, rows[at] * pot_wide[n, at], LOW))
                    keep = row_live[side, 2 * b + j, pl.ds(n, 1), :]
                    for player in range(2):
                        total = jnp.sum(
                            best[player * GROUPS : (player + 1) * GROUPS], axis=0, keepdims=True
                        )
                        river[side, b, player, j, pl.ds(n, 1), :] = total * keep

        return carry

    steps = TALL // PAIR
    for b in range(blocks):
        for span in range(spans):
            if b == 0:
                peer_copy(span).wait_recv()
                spread_lines(1 - hand, span)
            lax.fori_loop(span * steps, (span + 1) * steps, functools.partial(one_step, b), 0)
            if b > 0 and span == 0:
                sum_block(b - 1)
            if b > 0 and span == spans - 1:
                pass_block(b - 1)
        river_copy(b).start()
    sum_block(blocks - 1)
    pass_block(blocks - 1)

    for b in range(blocks):
        for offset in range(1, high):
            line_copy(b, offset, True).wait_recv()
    kind = lax.rem(lax.broadcasted_iota(jnp.int32, (2 * TACT, WIDE), 0), TACT)
    share = jnp.zeros((1, WIDE), f32)
    for row in range(high):
        for t in range(turns_mine):
            turn = (row * low + q) * turns_mine + t
            at = slice(t * 2 * TACT, (t + 1) * 2 * TACT)
            for b in range(blocks):
                width = min(WIDE, half - b * WIDE)
                cut = slice(b * WIDE, b * WIDE + width)
                total = got_line[b, 0, row, at]
                for other in range(1, high):
                    total = total + got_line[b, other, row, at]
                total = jnp.where(kind < turn_legal[turn], total, LOW)
                for player in range(2):
                    best = jnp.max(
                        total[player * TACT : (player + 1) * TACT], axis=0, keepdims=True
                    )[:, :width]
                    found[row, t, player : player + 1, cut] = best
                    part_of = reach[turn, player : player + 1, cut] * best
                    if width < WIDE:
                        part_of = jnp.concatenate(
                            [part_of, jnp.zeros((1, WIDE - width), f32)], axis=1
                        )
                    share = share + part_of
    best_out[...] = found[z]
    me = q * 2 + hand
    shares[me] = jnp.broadcast_to(jnp.sum(share, axis=1, keepdims=True), (1, LANE))

    def tell_plane(offset, back):
        to, device = plane_device(offset)
        source = lax.rem(me + 2 * low - offset, 2 * low) if back else me
        return pltpu.make_async_remote_copy(
            src_ref=shares.at[me],
            dst_ref=shares.at[source],
            send_sem=tell_send.at[offset - 1],
            recv_sem=tell_recv.at[offset - 1],
            device_id=device,
            device_id_type=MESH,
        )

    for offset in range(1, 2 * low):
        tell_plane(offset, False).start()
    for offset in range(1, 2 * low):
        tell_plane(offset, True).wait_recv()
    whole = shares[0]
    for spot in range(1, 2 * low):
        whole = whole + shares[spot]
    total_out[0, 0] = whole[0, 0]

    for span in range(spans):
        peer_copy(span).wait_send()
    for b in range(blocks):
        river_copy(b).wait_send()
        for offset in range(1, low):
            plane_copy(b, offset).wait_send()
        for offset in range(1, high):
            line_copy(b, offset).wait_send()
    for offset in range(1, 2 * low):
        tell_plane(offset, False).wait_send()


def solution(mesh):
    n_node = mesh.shape["node"]
    high = min(4, n_node)
    low = n_node // high

    def local(
        ranges, strengths, live_hands, pot_sizes, action_counts, parents, turn_counts, root_reach
    ):
        nodes, line_rows, half = ranges.shape
        hands = strengths.shape[1]
        tiles = -(-half // WIDE) * 2
        blocks = tiles // 2
        turns_all = turn_counts.shape[0]
        turns_mine = turns_all // n_node
        rows_all = turns_all * 2 * TACT
        out_rows = turns_mine * 2 * TACT
        mine = nodes // 2
        spans = mine // TALL
        f32, bf16 = jnp.float32, jnp.bfloat16
        vmem = pl.BlockSpec(memory_space=pltpu.VMEM)
        smem = pl.BlockSpec(memory_space=pltpu.SMEM)
        hbm = pl.BlockSpec(memory_space=pl.ANY)
        dma = pltpu.SemaphoreType.DMA
        sizes = (n_node, low, high, nodes, half, tiles, turns_mine, rows_all)
        best, total = pl.pallas_call(
            functools.partial(kernel, sizes),
            out_shape=(
                jax.ShapeDtypeStruct((turns_mine, 2, half), f32),
                jax.ShapeDtypeStruct((1, 1), f32),
            ),
            in_specs=[hbm, vmem, vmem, vmem, smem, vmem, smem, vmem, hbm],
            out_specs=(vmem, smem),
            scratch_shapes=[
                pltpu.VMEM((2, spans, tiles * LANE, TALL, line_rows), bf16),
                [pltpu.VMEM((LANE * TALL, line_rows), f32) for _ in range(2)],
                pltpu.VMEM((mine, 2 * tiles, line_rows, LANE), bf16),
                pltpu.VMEM((2, tiles, LANE, LANE), f32),
                pltpu.VMEM((2, tiles, mine, LANE), f32),
                pltpu.VMEM((2 * tiles, LANE, LANE), f32),
                pltpu.VMEM((mine, 2 * tiles * LANE, LANE), bf16),
                pltpu.VMEM((2 * tiles, 2 * tiles * LANE, LANE), jnp.int8),
                pltpu.VMEM((2 * tiles, 2 * tiles * LANE, LANE), bf16),
                pltpu.VMEM((mine, line_rows, LANE), f32),
                [pltpu.VMEM((line_rows, LANE), f32) for _ in range(2 * TALL)],
                pltpu.VMEM((2, blocks, 2, 2, mine, LANE), f32),
                pltpu.VMEM((blocks, 2, 2, mine, LANE), f32),
                pltpu.VMEM((rows_all, 12 * mine), bf16),
                pltpu.VMEM((blocks, low, high, out_rows, WIDE), f32),
                pltpu.VMEM((blocks, low - 1, high, out_rows, WIDE), f32),
                pltpu.VMEM((blocks, high, high, out_rows, WIDE), f32),
                pltpu.VMEM((high, turns_mine, 2, half), f32),
                pltpu.VMEM((2 * low, 1, LANE), f32),
                dma,
                dma((spans,)),
                dma((spans,)),
                dma((spans,)),
                dma((blocks,)),
                dma((blocks,)),
                dma((blocks, low - 1)),
                dma((blocks, low - 1)),
                dma((blocks, high - 1)),
                dma((blocks, high - 1)),
                dma((2 * low - 1,)),
                dma((2 * low - 1,)),
            ],
            compiler_params=pltpu.CompilerParams(
                collective_id=0, has_side_effects=True, vmem_limit_bytes=60 * 1024 * 1024
            ),
        )(
            jnp.transpose(ranges, (2, 0, 1)),
            strengths,
            live_hands,
            pot_sizes,
            action_counts,
            parents.reshape(1, nodes),
            turn_counts,
            root_reach,
            compat_table(hands, half, tiles),
        )
        return best, total.reshape(())

    in_specs = (
        P("node", None, "hand"),
        P("node", None),
        P("node", None),
        P("node", None),
        P("node"),
        P("node"),
        P(),
        P(None, None, "hand"),
    )
    out_specs = (P("node", None, "hand"), P())
    return jax.shard_map(local, mesh=mesh, in_specs=in_specs, out_specs=out_specs, check_vma=False)
```

```python
import functools

import jax
import jax.numpy as jnp
import numpy as np
from jax import lax
from jax.experimental import pallas as pl
from jax.experimental.pallas import tpu as pltpu
from jax.sharding import PartitionSpec as P

ACT = 8
GROUPS = 8
TACT = 4
LANE = 128
PACK = 16
WIDE = 256
TALL = 8
PAIR = 4
MESH = pl.DeviceIdType.MESH
MID = 200.0
LOW = -1e30


def compat_table(hands, half, tiles):
    pairs = [(a, b) for a in range(52) for b in range(a + 1, 52)][:hands]
    holds = np.zeros((hands, 52), np.int32)
    for hand, (a, b) in enumerate(pairs):
        holds[hand, a] = holds[hand, b] = 1
    apart = (holds @ holds.T) == 0
    table = np.zeros((2, tiles * LANE, 2, tiles * LANE), np.int8)
    table[:, :half, :, :half] = apart.reshape(2, half, 2, half)
    table = table.reshape(2 * tiles * LANE, 2 * tiles, LANE).transpose(1, 0, 2)
    return jnp.asarray(table)


def kernel(
    sizes,
    ranges,
    strengths,
    live,
    pots,
    legal,
    parents,
    turn_legal,
    reach,
    table,
    best_out,
    total_out,
    raw,
    loose,
    lines,
    row_s,
    row_live,
    col_s,
    wide,
    small,
    pot_wide,
    turned,
    river,
    river_in,
    chosen,
    part,
    got_plane,
    got_line,
    found,
    shares,
    table_sem,
    local_sem,
    send_sem,
    recv_sem,
    river_send,
    river_recv,
    plane_send,
    plane_recv,
    line_send,
    line_recv,
    tell_send,
    tell_recv,
):
    n_node, low, high, nodes, half, tiles, turns_mine, rows_all = sizes
    f32, bf16 = jnp.float32, jnp.bfloat16
    node = lax.axis_index("node")
    hand = lax.axis_index("hand")
    q = lax.rem(node, low)
    z = node // low
    mine = nodes // 2
    spans = mine // TALL
    blocks = tiles // 2
    rows_k = tiles * LANE
    used = -(-half // PACK) * PACK
    first_row = pl.multiple_of(hand * mine, TALL)
    each = 2 * GROUPS
    line_rows = each * ACT
    out_rows = turns_mine * 2 * TACT

    barrier = pltpu.get_barrier_semaphore()

    def plane_device(offset):
        spot = lax.rem(q * 2 + hand + offset, 2 * low)
        return spot, (z * low + spot // 2, lax.rem(spot, 2))

    def line_device(offset):
        spot = lax.rem(z + offset, high)
        return spot, (spot * low + q, hand)

    for offset in range(1, 2 * low):
        pl.semaphore_signal(
            barrier, inc=1, device_id=plane_device(offset)[1], device_id_type=MESH
        )
    for offset in range(1, high):
        pl.semaphore_signal(
            barrier, inc=1, device_id=line_device(offset)[1], device_id_type=MESH
        )

    def local_copy(span):
        at = pl.multiple_of(hand * mine + span * TALL, TALL)
        return pltpu.make_async_copy(
            ranges.at[:, pl.ds(at, TALL), :],
            raw.at[hand, span, pl.ds(0, half)],
            local_sem.at[span],
        )

    def peer_copy(span):
        at = pl.multiple_of((1 - hand) * mine + span * TALL, TALL)
        return pltpu.make_async_remote_copy(
            src_ref=ranges.at[:, pl.ds(at, TALL), :],
            dst_ref=raw.at[hand, span, pl.ds(0, half)],
            send_sem=send_sem.at[span],
            recv_sem=recv_sem.at[span],
            device_id=(node, 1 - hand),
            device_id_type=MESH,
        )

    table_copy = pltpu.make_async_copy(table, small, table_sem)
    for span in range(spans):
        local_copy(span).start()
    table_copy.start()

    for side in range(2):
        for span in range(spans):
            raw[side, span, half:] = jnp.zeros((rows_k - half, TALL, LANE), bf16)

    row_s[...] = jnp.zeros_like(row_s)
    row_live[...] = jnp.zeros_like(row_live)
    strength = strengths[pl.ds(first_row, mine), :].astype(f32) - MID
    alive = live[pl.ds(first_row, mine), :].astype(f32)
    for side in range(2):
        for tile in range(tiles):
            width = min(LANE, half - tile * LANE)
            cut = slice(side * half + tile * LANE, side * half + tile * LANE + width)
            row_s[side, tile, :mine, :width] = strength[:, cut]
            row_live[side, tile, :, :width] = alive[:, cut]

    pl.semaphore_wait(barrier, 2 * low - 1 + high - 1)
    for span in range(spans):
        peer_copy(span).start()

    def turn_rows(tile, carry):
        for side in range(2):
            col_s[side * tiles + tile] = row_s[side, tile].T
        return carry

    lax.fori_loop(0, tiles, turn_rows, 0)

    table_copy.wait()

    def compat_rows(tile, carry):
        at = pl.ds(pl.multiple_of(tile * LANE, LANE), LANE)
        for n in range(mine):
            spread = jnp.broadcast_to(col_s[tile, :, n : n + 1], (LANE, LANE))
            wide[n, at, :] = spread.astype(bf16)
        return carry

    lax.fori_loop(0, 2 * tiles, compat_rows, 0)

    pot_block = jnp.concatenate(
        [pots[pl.ds(first_row, mine), :], jnp.zeros((LANE - mine, line_rows), f32)], axis=0
    ).T
    turned[0][...] = pot_block
    for a in range(ACT):
        rows = turned[0][pl.ds(a, each, stride=ACT), :]
        for n in range(mine):
            pot_wide[n, a * each : (a + 1) * each] = jnp.broadcast_to(rows[:, n : n + 1], (each, LANE))

    group = 2 * mine
    depth = 2 * 3 * group
    source = lax.broadcasted_iota(jnp.int32, (group, depth), 0)
    column_at = lax.broadcasted_iota(jnp.int32, (group, depth), 1)
    owner = lax.rem(lax.rem(column_at, group) + hand * mine, group)
    pick = jnp.where(source == owner, 1.0, 0.0).astype(bf16)
    parent_rows = jnp.broadcast_to(parents[...].astype(f32), (16, nodes)).astype(bf16)
    parent_of = jnp.dot(parent_rows, pick, preferred_element_type=f32)[:1]
    row_at = lax.broadcasted_iota(jnp.int32, (rows_all, depth), 0)
    depth_at = lax.broadcasted_iota(jnp.int32, (rows_all, depth), 1)
    wanted = (row_at // (2 * TACT)) * TACT + lax.rem(row_at, TACT)
    same = lax.rem(row_at // TACT, 2) == depth_at // (3 * group)
    match = jnp.broadcast_to(parent_of, (rows_all, depth)) == wanted.astype(f32)
    chosen[...] = jnp.where(match & same, 1.0, 0.0).astype(bf16)

    def spread_lines(side, span):
        for tile in range(tiles):
            width = min(LANE, -(-(half - tile * LANE) // PACK) * PACK)
            bank = tile % 2
            block = raw[side, span, tile * LANE : tile * LANE + width].astype(f32)
            loose[bank][: width * TALL] = block.reshape(width * TALL, LANE)
            for u in range(TALL):
                n = span * TALL + u
                turn = turned[bank * TALL + u]
                turn[:, :width] = loose[bank][pl.ds(u, width, stride=TALL), :].T
                keep = row_live[side, tile, pl.ds(n, 1), :width]
                for a in range(ACT):
                    rows = turn[pl.ds(a, each, stride=ACT), :][:, :width] * keep
                    at = slice(a * each, (a + 1) * each)
                    lines[n, side * tiles + tile, at, :width] = rows.astype(bf16)

    for n in range(mine):
        for side in range(2):
            lines[n, side * tiles + half // LANE] = jnp.zeros((line_rows, LANE), bf16)

    def own_span(span, carry):
        local_copy(span).wait()
        spread_lines(hand, span)
        return carry

    lax.fori_loop(0, spans, own_span, 0)

    def river_copy(b):
        return pltpu.make_async_remote_copy(
            src_ref=river.at[1 - hand, b],
            dst_ref=river_in.at[b],
            send_sem=river_send.at[b],
            recv_sem=river_recv.at[b],
            device_id=(node, 1 - hand),
            device_id_type=MESH,
        )

    def plane_copy(b, offset):
        spot = lax.rem(q + offset, low)
        return pltpu.make_async_remote_copy(
            src_ref=part.at[b, spot],
            dst_ref=got_plane.at[b, offset - 1],
            send_sem=plane_send.at[b, offset - 1],
            recv_sem=plane_recv.at[b, offset - 1],
            device_id=(z * low + spot, hand),
            device_id_type=MESH,
        )

    def line_copy(b, offset, back=False):
        spot, device = line_device(offset)
        source = lax.rem(z + high - offset, high) if back else z
        return pltpu.make_async_remote_copy(
            src_ref=got_line.at[b, z],
            dst_ref=got_line.at[b, source],
            send_sem=line_send.at[b, offset - 1],
            recv_sem=line_recv.at[b, offset - 1],
            device_id=device,
            device_id_type=MESH,
        )

    def sum_block(b):
        river_copy(b).wait_recv()
        pieces = []
        for player in range(2):
            rest = jnp.concatenate(
                [
                    jnp.concatenate([river[hand, b, player, j], river_in[b, player, j]], axis=0)
                    for j in range(2)
                ],
                axis=1,
            )
            for _ in range(3):
                piece = rest.astype(bf16)
                pieces.append(piece)
                rest = rest - piece.astype(f32)
        sums = jnp.dot(
            chosen[...], jnp.concatenate(pieces, axis=0), preferred_element_type=f32
        )
        for other in range(n_node):
            part[b, other % low, other // low] = sums[other * out_rows : (other + 1) * out_rows]
        for offset in range(1, low):
            plane_copy(b, offset).start()

    def pass_block(b):
        whole = part[b, q]
        for offset in range(1, low):
            plane_copy(b, offset).wait_recv()
            whole = whole + got_plane[b, offset - 1]
        got_line[b, z] = whole
        for offset in range(1, high):
            line_copy(b, offset).start()

    def one_step(b, p, carry):
        for u in range(PAIR):
            n = p * PAIR + u
            left = jnp.concatenate([lines[n, k] for k in range(2 * tiles)], axis=1)
            columns = []
            for side in range(2):
                for j in range(2):
                    hero = row_s[side, 2 * b + j, pl.ds(n, 1), :]
                    hero = jnp.broadcast_to(hero, (PACK, LANE)).astype(bf16)
                    hero = jnp.concatenate([hero] * (used // PACK), axis=0)
                    stack = []
                    for other in range(2):
                        at = slice(other * rows_k, other * rows_k + used)
                        upper = small[side * tiles + 2 * b + j, at, :].astype(bf16)
                        gap = hero - wide[n, at, :]
                        stack.append(lax.clamp(jnp.bfloat16(-1), gap * upper, jnp.bfloat16(1)))
                        if rows_k > used:
                            stack.append(jnp.zeros((rows_k - used, LANE), bf16))
                    columns.append(jnp.concatenate(stack, axis=0))
            signs = jnp.concatenate(columns, axis=1)
            result = jnp.dot(left, signs, preferred_element_type=f32)
            count = legal[hand * mine + n]
            for side in range(2):
                for j in range(2):
                    spot = side * 2 + j
                    rows = result[:, spot * LANE : (spot + 1) * LANE]
                    best = rows[:each] * pot_wide[n, :each]
                    for a in range(1, ACT):
                        at = slice(a * each, (a + 1) * each)
                        best = jnp.maximum(best, jnp.where(a < count, rows[at] * pot_wide[n, at], LOW))
                    keep = row_live[side, 2 * b + j, pl.ds(n, 1), :]
                    for player in range(2):
                        total = jnp.sum(
                            best[player * GROUPS : (player + 1) * GROUPS], axis=0, keepdims=True
                        )
                        river[side, b, player, j, pl.ds(n, 1), :] = total * keep

        return carry

    steps = TALL // PAIR
    for b in range(blocks):
        for span in range(spans):
            if b == 0:
                peer_copy(span).wait_recv()
                spread_lines(1 - hand, span)
            lax.fori_loop(span * steps, (span + 1) * steps, functools.partial(one_step, b), 0)
            if b > 0 and span == 0:
                sum_block(b - 1)
            if b > 0 and span == spans - 1:
                pass_block(b - 1)
        river_copy(b).start()
    sum_block(blocks - 1)
    pass_block(blocks - 1)

    for b in range(blocks):
        for offset in range(1, high):
            line_copy(b, offset, True).wait_recv()
    kind = lax.rem(lax.broadcasted_iota(jnp.int32, (2 * TACT, WIDE), 0), TACT)
    share = jnp.zeros((1, WIDE), f32)
    for row in range(high):
        for t in range(turns_mine):
            turn = (row * low + q) * turns_mine + t
            at = slice(t * 2 * TACT, (t + 1) * 2 * TACT)
            for b in range(blocks):
                width = min(WIDE, half - b * WIDE)
                cut = slice(b * WIDE, b * WIDE + width)
                total = got_line[b, 0, row, at]
                for other in range(1, high):
                    total = total + got_line[b, other, row, at]
                total = jnp.where(kind < turn_legal[turn], total, LOW)
                for player in range(2):
                    best = jnp.max(
                        total[player * TACT : (player + 1) * TACT], axis=0, keepdims=True
                    )[:, :width]
                    found[row, t, player : player + 1, cut] = best
                    part_of = reach[turn, player : player + 1, cut] * best
                    if width < WIDE:
                        part_of = jnp.concatenate(
                            [part_of, jnp.zeros((1, WIDE - width), f32)], axis=1
                        )
                    share = share + part_of
    best_out[...] = found[z]
    me = q * 2 + hand
    shares[me] = jnp.broadcast_to(jnp.sum(share, axis=1, keepdims=True), (1, LANE))

    def tell_plane(offset, back):
        to, device = plane_device(offset)
        source = lax.rem(me + 2 * low - offset, 2 * low) if back else me
        return pltpu.make_async_remote_copy(
            src_ref=shares.at[me],
            dst_ref=shares.at[source],
            send_sem=tell_send.at[offset - 1],
            recv_sem=tell_recv.at[offset - 1],
            device_id=device,
            device_id_type=MESH,
        )

    for offset in range(1, 2 * low):
        tell_plane(offset, False).start()
    for offset in range(1, 2 * low):
        tell_plane(offset, True).wait_recv()
    whole = shares[0]
    for spot in range(1, 2 * low):
        whole = whole + shares[spot]
    total_out[0, 0] = whole[0, 0]

    for span in range(spans):
        peer_copy(span).wait_send()
    for b in range(blocks):
        river_copy(b).wait_send()
        for offset in range(1, low):
            plane_copy(b, offset).wait_send()
        for offset in range(1, high):
            line_copy(b, offset).wait_send()
    for offset in range(1, 2 * low):
        tell_plane(offset, False).wait_send()


def solution(mesh):
    n_node = mesh.shape["node"]
    high = min(4, n_node)
    low = n_node // high

    def local(
        ranges, strengths, live_hands, pot_sizes, action_counts, parents, turn_counts, root_reach
    ):
        nodes, line_rows, half = ranges.shape
        hands = strengths.shape[1]
        tiles = -(-half // WIDE) * 2
        blocks = tiles // 2
        turns_all = turn_counts.shape[0]
        turns_mine = turns_all // n_node
        rows_all = turns_all * 2 * TACT
        out_rows = turns_mine * 2 * TACT
        mine = nodes // 2
        spans = mine // TALL
        f32, bf16 = jnp.float32, jnp.bfloat16
        vmem = pl.BlockSpec(memory_space=pltpu.VMEM)
        smem = pl.BlockSpec(memory_space=pltpu.SMEM)
        hbm = pl.BlockSpec(memory_space=pl.ANY)
        dma = pltpu.SemaphoreType.DMA
        sizes = (n_node, low, high, nodes, half, tiles, turns_mine, rows_all)
        best, total = pl.pallas_call(
            functools.partial(kernel, sizes),
            out_shape=(
                jax.ShapeDtypeStruct((turns_mine, 2, half), f32),
                jax.ShapeDtypeStruct((1, 1), f32),
            ),
            in_specs=[hbm, vmem, vmem, vmem, smem, vmem, smem, vmem, hbm],
            out_specs=(vmem, smem),
            scratch_shapes=[
                pltpu.VMEM((2, spans, tiles * LANE, TALL, line_rows), bf16),
                [pltpu.VMEM((LANE * TALL, line_rows), f32) for _ in range(2)],
                pltpu.VMEM((mine, 2 * tiles, line_rows, LANE), bf16),
                pltpu.VMEM((2, tiles, LANE, LANE), f32),
                pltpu.VMEM((2, tiles, mine, LANE), f32),
                pltpu.VMEM((2 * tiles, LANE, LANE), f32),
                pltpu.VMEM((mine, 2 * tiles * LANE, LANE), bf16),
                pltpu.VMEM((2 * tiles, 2 * tiles * LANE, LANE), jnp.int8),
                pltpu.VMEM((mine, line_rows, LANE), f32),
                [pltpu.VMEM((line_rows, LANE), f32) for _ in range(2 * TALL)],
                pltpu.VMEM((2, blocks, 2, 2, mine, LANE), f32),
                pltpu.VMEM((blocks, 2, 2, mine, LANE), f32),
                pltpu.VMEM((rows_all, 12 * mine), bf16),
                pltpu.VMEM((blocks, low, high, out_rows, WIDE), f32),
                pltpu.VMEM((blocks, low - 1, high, out_rows, WIDE), f32),
                pltpu.VMEM((blocks, high, high, out_rows, WIDE), f32),
                pltpu.VMEM((high, turns_mine, 2, half), f32),
                pltpu.VMEM((2 * low, 1, LANE), f32),
                dma,
                dma((spans,)),
                dma((spans,)),
                dma((spans,)),
                dma((blocks,)),
                dma((blocks,)),
                dma((blocks, low - 1)),
                dma((blocks, low - 1)),
                dma((blocks, high - 1)),
                dma((blocks, high - 1)),
                dma((2 * low - 1,)),
                dma((2 * low - 1,)),
            ],
            compiler_params=pltpu.CompilerParams(
                collective_id=0, has_side_effects=True, vmem_limit_bytes=60 * 1024 * 1024
            ),
        )(
            jnp.transpose(ranges, (2, 0, 1)),
            strengths,
            live_hands,
            pot_sizes,
            action_counts,
            parents.reshape(1, nodes),
            turn_counts,
            root_reach,
            compat_table(hands, half, tiles),
        )
        return best, total.reshape(())

    in_specs = (
        P("node", None, "hand"),
        P("node", None),
        P("node", None),
        P("node", None),
        P("node"),
        P("node"),
        P(),
        P(None, None, "hand"),
    )
    out_specs = (P("node", None, "hand"), P())
    return jax.shard_map(local, mesh=mesh, in_specs=in_specs, out_specs=out_specs, check_vma=False)
```

```python
import functools

import jax
import jax.numpy as jnp
import numpy as np
from jax import lax
from jax.experimental import pallas as pl
from jax.experimental.pallas import tpu as pltpu
from jax.sharding import PartitionSpec as P

ACT = 8
GROUPS = 8
TACT = 4
LANE = 128
PACK = 16
WIDE = 256
TALL = 8
PAIR = 4
MESH = pl.DeviceIdType.MESH
MID = 200.0
LOW = -1e30


def compat_table(hands, half, tiles):
    pairs = [(a, b) for a in range(52) for b in range(a + 1, 52)][:hands]
    holds = np.zeros((hands, 52), np.int32)
    for hand, (a, b) in enumerate(pairs):
        holds[hand, a] = holds[hand, b] = 1
    apart = (holds @ holds.T) == 0
    table = np.zeros((2, tiles * LANE, 2, tiles * LANE), np.int8)
    table[:, :half, :, :half] = apart.reshape(2, half, 2, half)
    table = table.reshape(2 * tiles * LANE, 2 * tiles, LANE).transpose(1, 0, 2)
    return jnp.asarray(table)


def kernel(
    sizes,
    ranges,
    strengths,
    live,
    pots,
    legal,
    parents,
    turn_legal,
    reach,
    table,
    best_out,
    total_out,
    raw,
    loose,
    lines,
    row_s,
    row_live,
    wide,
    small,
    pot_wide,
    turned,
    river,
    river_in,
    chosen,
    part,
    got_plane,
    got_line,
    found,
    shares,
    table_sem,
    local_sem,
    send_sem,
    recv_sem,
    river_send,
    river_recv,
    plane_send,
    plane_recv,
    line_send,
    line_recv,
    tell_send,
    tell_recv,
):
    n_node, low, high, nodes, half, tiles, turns_mine, rows_all = sizes
    f32, bf16 = jnp.float32, jnp.bfloat16
    node = lax.axis_index("node")
    hand = lax.axis_index("hand")
    q = lax.rem(node, low)
    z = node // low
    mine = nodes // 2
    spans = mine // TALL
    blocks = tiles // 2
    rows_k = tiles * LANE
    used = -(-half // PACK) * PACK
    first_row = pl.multiple_of(hand * mine, TALL)
    each = 2 * GROUPS
    line_rows = each * ACT
    out_rows = turns_mine * 2 * TACT

    barrier = pltpu.get_barrier_semaphore()

    def plane_device(offset):
        spot = lax.rem(q * 2 + hand + offset, 2 * low)
        return spot, (z * low + spot // 2, lax.rem(spot, 2))

    def line_device(offset):
        spot = lax.rem(z + offset, high)
        return spot, (spot * low + q, hand)

    for offset in range(1, 2 * low):
        pl.semaphore_signal(
            barrier, inc=1, device_id=plane_device(offset)[1], device_id_type=MESH
        )
    for offset in range(1, high):
        pl.semaphore_signal(
            barrier, inc=1, device_id=line_device(offset)[1], device_id_type=MESH
        )

    def local_copy(span):
        at = pl.multiple_of(hand * mine + span * TALL, TALL)
        return pltpu.make_async_copy(
            ranges.at[:, pl.ds(at, TALL), :],
            raw.at[hand, span, pl.ds(0, half)],
            local_sem.at[span],
        )

    def peer_copy(span):
        at = pl.multiple_of((1 - hand) * mine + span * TALL, TALL)
        return pltpu.make_async_remote_copy(
            src_ref=ranges.at[:, pl.ds(at, TALL), :],
            dst_ref=raw.at[hand, span, pl.ds(0, half)],
            send_sem=send_sem.at[span],
            recv_sem=recv_sem.at[span],
            device_id=(node, 1 - hand),
            device_id_type=MESH,
        )

    table_copy = pltpu.make_async_copy(table, small, table_sem)
    for span in range(spans):
        local_copy(span).start()
    table_copy.start()

    for side in range(2):
        for span in range(spans):
            raw[side, span, half:] = jnp.zeros((rows_k - half, TALL, LANE), bf16)

    row_s[...] = jnp.zeros_like(row_s)
    row_live[...] = jnp.zeros_like(row_live)
    strength = strengths[pl.ds(first_row, mine), :].astype(f32) - MID
    alive = live[pl.ds(first_row, mine), :].astype(f32)
    for side in range(2):
        for tile in range(tiles):
            width = min(LANE, half - tile * LANE)
            cut = slice(side * half + tile * LANE, side * half + tile * LANE + width)
            row_s[side, tile, :mine, :width] = strength[:, cut]
            row_live[side, tile, :, :width] = alive[:, cut]

    pl.semaphore_wait(barrier, 2 * low - 1 + high - 1)
    for span in range(spans):
        peer_copy(span).start()

    table_copy.wait()

    def wide_rows(tile, carry):
        at = pl.ds(pl.multiple_of(tile * LANE, LANE), LANE)
        for n in range(mine):
            block = jnp.broadcast_to(row_s[tile // tiles, lax.rem(tile, tiles), n : n + 1, :], (LANE, LANE))
            wide[n, at, :] = block.astype(bf16).T
        return carry

    lax.fori_loop(0, 2 * tiles, wide_rows, 0)

    pot_block = jnp.concatenate(
        [pots[pl.ds(first_row, mine), :], jnp.zeros((LANE - mine, line_rows), f32)], axis=0
    ).T
    turned[0][...] = pot_block
    for a in range(ACT):
        rows = turned[0][pl.ds(a, each, stride=ACT), :]
        for n in range(mine):
            pot_wide[n, a * each : (a + 1) * each] = jnp.broadcast_to(rows[:, n : n + 1], (each, LANE))

    group = 2 * mine
    depth = 2 * 3 * group
    source = lax.broadcasted_iota(jnp.int32, (group, depth), 0)
    column_at = lax.broadcasted_iota(jnp.int32, (group, depth), 1)
    owner = lax.rem(lax.rem(column_at, group) + hand * mine, group)
    pick = jnp.where(source == owner, 1.0, 0.0).astype(bf16)
    parent_rows = jnp.broadcast_to(parents[...].astype(f32), (16, nodes)).astype(bf16)
    parent_of = jnp.dot(parent_rows, pick, preferred_element_type=f32)[:1]
    row_at = lax.broadcasted_iota(jnp.int32, (rows_all, depth), 0)
    depth_at = lax.broadcasted_iota(jnp.int32, (rows_all, depth), 1)
    wanted = (row_at // (2 * TACT)) * TACT + lax.rem(row_at, TACT)
    same = lax.rem(row_at // TACT, 2) == depth_at // (3 * group)
    match = jnp.broadcast_to(parent_of, (rows_all, depth)) == wanted.astype(f32)
    chosen[...] = jnp.where(match & same, 1.0, 0.0).astype(bf16)

    def spread_lines(side, span):
        for tile in range(tiles):
            width = min(LANE, -(-(half - tile * LANE) // PACK) * PACK)
            bank = tile % 2
            block = raw[side, span, tile * LANE : tile * LANE + width].astype(f32)
            loose[bank][: width * TALL] = block.reshape(width * TALL, LANE)
            for u in range(TALL):
                n = span * TALL + u
                turn = turned[bank * TALL + u]
                turn[:, :width] = loose[bank][pl.ds(u, width, stride=TALL), :].T
                keep = row_live[side, tile, pl.ds(n, 1), :width]
                for a in range(ACT):
                    rows = turn[pl.ds(a, each, stride=ACT), :][:, :width] * keep
                    at = slice(a * each, (a + 1) * each)
                    lines[n, side * tiles + tile, at, :width] = rows.astype(bf16)

    for n in range(mine):
        for side in range(2):
            lines[n, side * tiles + half // LANE] = jnp.zeros((line_rows, LANE), bf16)

    def own_span(span, carry):
        local_copy(span).wait()
        spread_lines(hand, span)
        return carry

    lax.fori_loop(0, spans, own_span, 0)

    def river_copy(b):
        return pltpu.make_async_remote_copy(
            src_ref=river.at[1 - hand, b],
            dst_ref=river_in.at[b],
            send_sem=river_send.at[b],
            recv_sem=river_recv.at[b],
            device_id=(node, 1 - hand),
            device_id_type=MESH,
        )

    def plane_copy(b, offset):
        spot = lax.rem(q + offset, low)
        return pltpu.make_async_remote_copy(
            src_ref=part.at[b, spot],
            dst_ref=got_plane.at[b, offset - 1],
            send_sem=plane_send.at[b, offset - 1],
            recv_sem=plane_recv.at[b, offset - 1],
            device_id=(z * low + spot, hand),
            device_id_type=MESH,
        )

    def line_copy(b, offset, back=False):
        spot, device = line_device(offset)
        source = lax.rem(z + high - offset, high) if back else z
        return pltpu.make_async_remote_copy(
            src_ref=got_line.at[b, z],
            dst_ref=got_line.at[b, source],
            send_sem=line_send.at[b, offset - 1],
            recv_sem=line_recv.at[b, offset - 1],
            device_id=device,
            device_id_type=MESH,
        )

    def sum_block(b):
        river_copy(b).wait_recv()
        pieces = []
        for player in range(2):
            rest = jnp.concatenate(
                [
                    jnp.concatenate([river[hand, b, player, j], river_in[b, player, j]], axis=0)
                    for j in range(2)
                ],
                axis=1,
            )
            for _ in range(3):
                piece = rest.astype(bf16)
                pieces.append(piece)
                rest = rest - piece.astype(f32)
        sums = jnp.dot(
            chosen[...], jnp.concatenate(pieces, axis=0), preferred_element_type=f32
        )
        for other in range(n_node):
            part[b, other % low, other // low] = sums[other * out_rows : (other + 1) * out_rows]
        for offset in range(1, low):
            plane_copy(b, offset).start()

    def pass_block(b):
        whole = part[b, q]
        for offset in range(1, low):
            plane_copy(b, offset).wait_recv()
            whole = whole + got_plane[b, offset - 1]
        got_line[b, z] = whole
        for offset in range(1, high):
            line_copy(b, offset).start()

    def one_step(b, p, carry):
        for u in range(PAIR):
            n = p * PAIR + u
            left = jnp.concatenate([lines[n, k] for k in range(2 * tiles)], axis=1)
            columns = []
            for side in range(2):
                for j in range(2):
                    hero = row_s[side, 2 * b + j, pl.ds(n, 1), :]
                    hero = jnp.broadcast_to(hero, (PACK, LANE)).astype(bf16)
                    hero = jnp.concatenate([hero] * (used // PACK), axis=0)
                    stack = []
                    for other in range(2):
                        at = slice(other * rows_k, other * rows_k + used)
                        upper = small[side * tiles + 2 * b + j, at, :].astype(bf16)
                        gap = hero - wide[n, at, :]
                        stack.append(lax.clamp(jnp.bfloat16(-1), gap * upper, jnp.bfloat16(1)))
                        if rows_k > used:
                            stack.append(jnp.zeros((rows_k - used, LANE), bf16))
                    columns.append(jnp.concatenate(stack, axis=0))
            signs = jnp.concatenate(columns, axis=1)
            result = jnp.dot(left, signs, preferred_element_type=f32)
            count = legal[hand * mine + n]
            for side in range(2):
                for j in range(2):
                    spot = side * 2 + j
                    rows = result[:, spot * LANE : (spot + 1) * LANE]
                    best = rows[:each] * pot_wide[n, :each]
                    for a in range(1, ACT):
                        at = slice(a * each, (a + 1) * each)
                        best = jnp.maximum(best, jnp.where(a < count, rows[at] * pot_wide[n, at], LOW))
                    keep = row_live[side, 2 * b + j, pl.ds(n, 1), :]
                    for player in range(2):
                        total = jnp.sum(
                            best[player * GROUPS : (player + 1) * GROUPS], axis=0, keepdims=True
                        )
                        river[side, b, player, j, pl.ds(n, 1), :] = total * keep

        return carry

    steps = TALL // PAIR
    for b in range(blocks):
        for span in range(spans):
            if b == 0:
                peer_copy(span).wait_recv()
                spread_lines(1 - hand, span)
            lax.fori_loop(span * steps, (span + 1) * steps, functools.partial(one_step, b), 0)
            if b > 0 and span == 0:
                sum_block(b - 1)
            if span == spans - 1:
                river_copy(b).start()
                if b > 0:
                    pass_block(b - 1)
    sum_block(blocks - 1)
    pass_block(blocks - 1)

    for b in range(blocks):
        for offset in range(1, high):
            line_copy(b, offset, True).wait_recv()
    kind = lax.rem(lax.broadcasted_iota(jnp.int32, (2 * TACT, WIDE), 0), TACT)
    share = jnp.zeros((1, WIDE), f32)
    for row in range(high):
        for t in range(turns_mine):
            turn = (row * low + q) * turns_mine + t
            at = slice(t * 2 * TACT, (t + 1) * 2 * TACT)
            for b in range(blocks):
                width = min(WIDE, half - b * WIDE)
                cut = slice(b * WIDE, b * WIDE + width)
                total = got_line[b, 0, row, at]
                for other in range(1, high):
                    total = total + got_line[b, other, row, at]
                total = jnp.where(kind < turn_legal[turn], total, LOW)
                for player in range(2):
                    best = jnp.max(
                        total[player * TACT : (player + 1) * TACT], axis=0, keepdims=True
                    )[:, :width]
                    found[row, t, player : player + 1, cut] = best
                    part_of = reach[turn, player : player + 1, cut] * best
                    if width < WIDE:
                        part_of = jnp.concatenate(
                            [part_of, jnp.zeros((1, WIDE - width), f32)], axis=1
                        )
                    share = share + part_of
    best_out[...] = found[z]
    me = q * 2 + hand
    shares[me] = jnp.broadcast_to(jnp.sum(share, axis=1, keepdims=True), (1, LANE))

    def tell_plane(offset, back):
        to, device = plane_device(offset)
        source = lax.rem(me + 2 * low - offset, 2 * low) if back else me
        return pltpu.make_async_remote_copy(
            src_ref=shares.at[me],
            dst_ref=shares.at[source],
            send_sem=tell_send.at[offset - 1],
            recv_sem=tell_recv.at[offset - 1],
            device_id=device,
            device_id_type=MESH,
        )

    for offset in range(1, 2 * low):
        tell_plane(offset, False).start()
    for offset in range(1, 2 * low):
        tell_plane(offset, True).wait_recv()
    whole = shares[0]
    for spot in range(1, 2 * low):
        whole = whole + shares[spot]
    total_out[0, 0] = whole[0, 0]

    for span in range(spans):
        peer_copy(span).wait_send()
    for b in range(blocks):
        river_copy(b).wait_send()
        for offset in range(1, low):
            plane_copy(b, offset).wait_send()
        for offset in range(1, high):
            line_copy(b, offset).wait_send()
    for offset in range(1, 2 * low):
        tell_plane(offset, False).wait_send()


def solution(mesh):
    n_node = mesh.shape["node"]
    high = min(4, n_node)
    low = n_node // high

    def local(
        ranges, strengths, live_hands, pot_sizes, action_counts, parents, turn_counts, root_reach
    ):
        nodes, line_rows, half = ranges.shape
        hands = strengths.shape[1]
        tiles = -(-half // WIDE) * 2
        blocks = tiles // 2
        turns_all = turn_counts.shape[0]
        turns_mine = turns_all // n_node
        rows_all = turns_all * 2 * TACT
        out_rows = turns_mine * 2 * TACT
        mine = nodes // 2
        spans = mine // TALL
        f32, bf16 = jnp.float32, jnp.bfloat16
        vmem = pl.BlockSpec(memory_space=pltpu.VMEM)
        smem = pl.BlockSpec(memory_space=pltpu.SMEM)
        hbm = pl.BlockSpec(memory_space=pl.ANY)
        dma = pltpu.SemaphoreType.DMA
        sizes = (n_node, low, high, nodes, half, tiles, turns_mine, rows_all)
        best, total = pl.pallas_call(
            functools.partial(kernel, sizes),
            out_shape=(
                jax.ShapeDtypeStruct((turns_mine, 2, half), f32),
                jax.ShapeDtypeStruct((1, 1), f32),
            ),
            in_specs=[hbm, vmem, vmem, vmem, smem, vmem, smem, vmem, hbm],
            out_specs=(vmem, smem),
            scratch_shapes=[
                pltpu.VMEM((2, spans, tiles * LANE, TALL, line_rows), bf16),
                [pltpu.VMEM((LANE * TALL, line_rows), f32) for _ in range(2)],
                pltpu.VMEM((mine, 2 * tiles, line_rows, LANE), bf16),
                pltpu.VMEM((2, tiles, mine, LANE), f32),
                pltpu.VMEM((2, tiles, mine, LANE), f32),
                pltpu.VMEM((mine, 2 * tiles * LANE, LANE), bf16),
                pltpu.VMEM((2 * tiles, 2 * tiles * LANE, LANE), jnp.int8),
                pltpu.VMEM((mine, line_rows, LANE), f32),
                [pltpu.VMEM((line_rows, LANE), f32) for _ in range(2 * TALL)],
                pltpu.VMEM((2, blocks, 2, 2, mine, LANE), f32),
                pltpu.VMEM((blocks, 2, 2, mine, LANE), f32),
                pltpu.VMEM((rows_all, 12 * mine), bf16),
                pltpu.VMEM((blocks, low, high, out_rows, WIDE), f32),
                pltpu.VMEM((blocks, low - 1, high, out_rows, WIDE), f32),
                pltpu.VMEM((blocks, high, high, out_rows, WIDE), f32),
                pltpu.VMEM((high, turns_mine, 2, half), f32),
                pltpu.VMEM((2 * low, 1, LANE), f32),
                dma,
                dma((spans,)),
                dma((spans,)),
                dma((spans,)),
                dma((blocks,)),
                dma((blocks,)),
                dma((blocks, low - 1)),
                dma((blocks, low - 1)),
                dma((blocks, high - 1)),
                dma((blocks, high - 1)),
                dma((2 * low - 1,)),
                dma((2 * low - 1,)),
            ],
            compiler_params=pltpu.CompilerParams(
                collective_id=0, has_side_effects=True, vmem_limit_bytes=60 * 1024 * 1024
            ),
        )(
            jnp.transpose(ranges, (2, 0, 1)),
            strengths,
            live_hands,
            pot_sizes,
            action_counts,
            parents.reshape(1, nodes),
            turn_counts,
            root_reach,
            compat_table(hands, half, tiles),
        )
        return best, total.reshape(())

    in_specs = (
        P("node", None, "hand"),
        P("node", None),
        P("node", None),
        P("node", None),
        P("node"),
        P("node"),
        P(),
        P(None, None, "hand"),
    )
    out_specs = (P("node", None, "hand"), P())
    return jax.shard_map(local, mesh=mesh, in_specs=in_specs, out_specs=out_specs, check_vma=False)
```

```python
import functools

import jax
import jax.numpy as jnp
import numpy as np
from jax import lax
from jax.experimental import pallas as pl
from jax.experimental.pallas import tpu as pltpu
from jax.sharding import PartitionSpec as P

ACT = 8
GROUPS = 8
TACT = 4
LANE = 128
PACK = 16
WIDE = 256
TALL = 8
PAIR = 4
MESH = pl.DeviceIdType.MESH
MID = 200.0
LOW = -1e30


def compat_table(hands, half, tiles):
    pairs = [(a, b) for a in range(52) for b in range(a + 1, 52)][:hands]
    holds = np.zeros((hands, 52), np.int32)
    for hand, (a, b) in enumerate(pairs):
        holds[hand, a] = holds[hand, b] = 1
    apart = (holds @ holds.T) == 0
    table = np.zeros((2, tiles * LANE, 2, tiles * LANE), np.int8)
    table[:, :half, :, :half] = apart.reshape(2, half, 2, half)
    table = table.reshape(2 * tiles * LANE, 2 * tiles, LANE).transpose(1, 0, 2)
    return jnp.asarray(table)


def kernel(
    sizes,
    ranges,
    strengths,
    live,
    pots,
    legal,
    parents,
    turn_legal,
    reach,
    table,
    best_out,
    total_out,
    raw,
    loose,
    lines,
    row_s,
    row_live,
    wide,
    small,
    pot_wide,
    turned,
    river,
    river_in,
    chosen,
    part,
    got_plane,
    got_line,
    found,
    shares,
    table_sem,
    local_sem,
    send_sem,
    recv_sem,
    river_send,
    river_recv,
    plane_send,
    plane_recv,
    line_send,
    line_recv,
    tell_send,
    tell_recv,
):
    n_node, low, high, nodes, half, tiles, turns_mine, rows_all = sizes
    f32, bf16 = jnp.float32, jnp.bfloat16
    node = lax.axis_index("node")
    hand = lax.axis_index("hand")
    q = lax.rem(node, low)
    z = node // low
    mine = nodes // 2
    spans = mine // TALL
    blocks = tiles // 2
    rows_k = tiles * LANE
    used = -(-half // PACK) * PACK
    first_row = pl.multiple_of(hand * mine, TALL)
    each = 2 * GROUPS
    line_rows = each * ACT
    out_rows = turns_mine * 2 * TACT

    barrier = pltpu.get_barrier_semaphore()

    def plane_device(offset):
        spot = lax.rem(q * 2 + hand + offset, 2 * low)
        return spot, (z * low + spot // 2, lax.rem(spot, 2))

    def line_device(offset):
        spot = lax.rem(z + offset, high)
        return spot, (spot * low + q, hand)

    for offset in range(1, 2 * low):
        pl.semaphore_signal(
            barrier, inc=1, device_id=plane_device(offset)[1], device_id_type=MESH
        )
    for offset in range(1, high):
        pl.semaphore_signal(
            barrier, inc=1, device_id=line_device(offset)[1], device_id_type=MESH
        )

    def local_copy(span):
        at = pl.multiple_of(hand * mine + span * TALL, TALL)
        return pltpu.make_async_copy(
            ranges.at[:, pl.ds(at, TALL), :],
            raw.at[hand, span, pl.ds(0, half)],
            local_sem.at[span],
        )

    def peer_copy(span):
        at = pl.multiple_of((1 - hand) * mine + span * TALL, TALL)
        return pltpu.make_async_remote_copy(
            src_ref=ranges.at[:, pl.ds(at, TALL), :],
            dst_ref=raw.at[hand, span, pl.ds(0, half)],
            send_sem=send_sem.at[span],
            recv_sem=recv_sem.at[span],
            device_id=(node, 1 - hand),
            device_id_type=MESH,
        )

    table_copy = pltpu.make_async_copy(table, small, table_sem)
    for span in range(spans):
        local_copy(span).start()
    table_copy.start()

    for side in range(2):
        for span in range(spans):
            if used > half:
                raw[side, span, half:used] = jnp.zeros((used - half, TALL, LANE), bf16)

    row_s[...] = jnp.zeros_like(row_s)
    row_live[...] = jnp.zeros_like(row_live)
    strength = strengths[pl.ds(first_row, mine), :].astype(f32) - MID
    alive = live[pl.ds(first_row, mine), :].astype(f32)
    for side in range(2):
        for tile in range(tiles):
            width = min(LANE, half - tile * LANE)
            cut = slice(side * half + tile * LANE, side * half + tile * LANE + width)
            row_s[side, tile, :mine, :width] = strength[:, cut]
            row_live[side, tile, :, :width] = alive[:, cut]

    pl.semaphore_wait(barrier, 2 * low - 1 + high - 1)
    for span in range(spans):
        peer_copy(span).start()

    table_copy.wait()

    def wide_rows(tile, carry):
        at = pl.ds(pl.multiple_of(tile * LANE, LANE), LANE)
        for n in range(mine):
            block = jnp.broadcast_to(row_s[tile // tiles, lax.rem(tile, tiles), n : n + 1, :], (LANE, LANE))
            wide[n, at, :] = block.astype(bf16).T
        return carry

    lax.fori_loop(0, 2 * tiles, wide_rows, 0)

    pot_block = jnp.concatenate(
        [pots[pl.ds(first_row, mine), :], jnp.zeros((LANE - mine, line_rows), f32)], axis=0
    ).T
    turned[0][...] = pot_block
    for a in range(ACT):
        rows = turned[0][pl.ds(a, each, stride=ACT), :]
        for n in range(mine):
            pot_wide[n, a * each : (a + 1) * each] = jnp.broadcast_to(rows[:, n : n + 1], (each, LANE))

    group = 2 * mine
    depth = 2 * 3 * group
    source = lax.broadcasted_iota(jnp.int32, (group, depth), 0)
    column_at = lax.broadcasted_iota(jnp.int32, (group, depth), 1)
    owner = lax.rem(lax.rem(column_at, group) + hand * mine, group)
    pick = jnp.where(source == owner, 1.0, 0.0).astype(bf16)
    parent_rows = jnp.broadcast_to(parents[...].astype(f32), (16, nodes)).astype(bf16)
    parent_of = jnp.dot(parent_rows, pick, preferred_element_type=f32)[:1]
    row_at = lax.broadcasted_iota(jnp.int32, (rows_all, depth), 0)
    depth_at = lax.broadcasted_iota(jnp.int32, (rows_all, depth), 1)
    wanted = (row_at // (2 * TACT)) * TACT + lax.rem(row_at, TACT)
    same = lax.rem(row_at // TACT, 2) == depth_at // (3 * group)
    match = jnp.broadcast_to(parent_of, (rows_all, depth)) == wanted.astype(f32)
    chosen[...] = jnp.where(match & same, 1.0, 0.0).astype(bf16)

    def spread_lines(side, span):
        for tile in range(tiles):
            width = min(LANE, -(-(half - tile * LANE) // PACK) * PACK)
            bank = tile % 2
            block = raw[side, span, tile * LANE : tile * LANE + width].astype(f32)
            loose[bank][: width * TALL] = block.reshape(width * TALL, LANE)
            for u in range(TALL):
                n = span * TALL + u
                turn = turned[bank * TALL + u]
                turn[:, :width] = loose[bank][pl.ds(u, width, stride=TALL), :].T
                keep = row_live[side, tile, pl.ds(n, 1), :width]
                for a in range(ACT):
                    rows = turn[pl.ds(a, each, stride=ACT), :][:, :width] * keep
                    at = slice(a * each, (a + 1) * each)
                    lines[n, side * tiles + tile, at, :width] = rows.astype(bf16)

    for n in range(mine):
        for side in range(2):
            lines[n, side * tiles + half // LANE] = jnp.zeros((line_rows, LANE), bf16)

    def own_span(span, carry):
        local_copy(span).wait()
        spread_lines(hand, span)
        return carry

    lax.fori_loop(0, spans, own_span, 0)

    def river_copy(b):
        return pltpu.make_async_remote_copy(
            src_ref=river.at[1 - hand, b],
            dst_ref=river_in.at[b],
            send_sem=river_send.at[b],
            recv_sem=river_recv.at[b],
            device_id=(node, 1 - hand),
            device_id_type=MESH,
        )

    def plane_copy(b, offset):
        spot = lax.rem(q + offset, low)
        return pltpu.make_async_remote_copy(
            src_ref=part.at[b, spot],
            dst_ref=got_plane.at[b, offset - 1],
            send_sem=plane_send.at[b, offset - 1],
            recv_sem=plane_recv.at[b, offset - 1],
            device_id=(z * low + spot, hand),
            device_id_type=MESH,
        )

    def line_copy(b, offset, back=False):
        spot, device = line_device(offset)
        source = lax.rem(z + high - offset, high) if back else z
        return pltpu.make_async_remote_copy(
            src_ref=got_line.at[b, z],
            dst_ref=got_line.at[b, source],
            send_sem=line_send.at[b, offset - 1],
            recv_sem=line_recv.at[b, offset - 1],
            device_id=device,
            device_id_type=MESH,
        )

    def sum_block(b):
        river_copy(b).wait_recv()
        pieces = []
        for player in range(2):
            rest = jnp.concatenate(
                [
                    jnp.concatenate([river[hand, b, player, j], river_in[b, player, j]], axis=0)
                    for j in range(2)
                ],
                axis=1,
            )
            for _ in range(3):
                piece = rest.astype(bf16)
                pieces.append(piece)
                rest = rest - piece.astype(f32)
        sums = jnp.dot(
            chosen[...], jnp.concatenate(pieces, axis=0), preferred_element_type=f32
        )
        for other in range(n_node):
            part[b, other % low, other // low] = sums[other * out_rows : (other + 1) * out_rows]
        for offset in range(1, low):
            plane_copy(b, offset).start()

    def pass_block(b):
        whole = part[b, q]
        for offset in range(1, low):
            plane_copy(b, offset).wait_recv()
            whole = whole + got_plane[b, offset - 1]
        got_line[b, z] = whole
        for offset in range(1, high):
            line_copy(b, offset).start()

    def one_step(b, p, carry):
        for u in range(PAIR):
            n = p * PAIR + u
            left = jnp.concatenate([lines[n, k] for k in range(2 * tiles)], axis=1)
            columns = []
            for side in range(2):
                for j in range(2):
                    hero = row_s[side, 2 * b + j, pl.ds(n, 1), :]
                    hero = jnp.broadcast_to(hero, (PACK, LANE)).astype(bf16)
                    hero = jnp.concatenate([hero] * (used // PACK), axis=0)
                    stack = []
                    for other in range(2):
                        at = slice(other * rows_k, other * rows_k + used)
                        upper = small[side * tiles + 2 * b + j, at, :].astype(bf16)
                        gap = hero - wide[n, at, :]
                        stack.append(lax.clamp(jnp.bfloat16(-1), gap * upper, jnp.bfloat16(1)))
                        if rows_k > used:
                            stack.append(jnp.zeros((rows_k - used, LANE), bf16))
                    columns.append(jnp.concatenate(stack, axis=0))
            signs = jnp.concatenate(columns, axis=1)
            result = jnp.dot(left, signs, preferred_element_type=f32)
            count = legal[hand * mine + n]
            for side in range(2):
                for j in range(2):
                    spot = side * 2 + j
                    rows = result[:, spot * LANE : (spot + 1) * LANE]
                    best = rows[:each] * pot_wide[n, :each]
                    for a in range(1, ACT):
                        at = slice(a * each, (a + 1) * each)
                        best = jnp.maximum(best, jnp.where(a < count, rows[at] * pot_wide[n, at], LOW))
                    keep = row_live[side, 2 * b + j, pl.ds(n, 1), :]
                    for player in range(2):
                        total = jnp.sum(
                            best[player * GROUPS : (player + 1) * GROUPS], axis=0, keepdims=True
                        )
                        river[side, b, player, j, pl.ds(n, 1), :] = total * keep

        return carry

    steps = TALL // PAIR
    for b in range(blocks):
        for span in range(spans):
            if b == 0:
                peer_copy(span).wait_recv()
                spread_lines(1 - hand, span)
            lax.fori_loop(span * steps, (span + 1) * steps, functools.partial(one_step, b), 0)
            if b > 0 and span == 0:
                sum_block(b - 1)
            if span == spans - 1:
                river_copy(b).start()
                if b > 0:
                    pass_block(b - 1)
    sum_block(blocks - 1)
    pass_block(blocks - 1)

    for b in range(blocks):
        for offset in range(1, high):
            line_copy(b, offset, True).wait_recv()
    kind = lax.rem(lax.broadcasted_iota(jnp.int32, (2 * TACT, WIDE), 0), TACT)
    share = jnp.zeros((1, WIDE), f32)
    for row in range(high):
        for t in range(turns_mine):
            turn = (row * low + q) * turns_mine + t
            at = slice(t * 2 * TACT, (t + 1) * 2 * TACT)
            for b in range(blocks):
                width = min(WIDE, half - b * WIDE)
                cut = slice(b * WIDE, b * WIDE + width)
                total = got_line[b, 0, row, at]
                for other in range(1, high):
                    total = total + got_line[b, other, row, at]
                total = jnp.where(kind < turn_legal[turn], total, LOW)
                for player in range(2):
                    best = jnp.max(
                        total[player * TACT : (player + 1) * TACT], axis=0, keepdims=True
                    )[:, :width]
                    found[row, t, player : player + 1, cut] = best
                    part_of = reach[turn, player : player + 1, cut] * best
                    if width < WIDE:
                        part_of = jnp.concatenate(
                            [part_of, jnp.zeros((1, WIDE - width), f32)], axis=1
                        )
                    share = share + part_of
    best_out[...] = found[z]
    me = q * 2 + hand
    shares[me] = jnp.broadcast_to(jnp.sum(share, axis=1, keepdims=True), (1, LANE))

    def tell_plane(offset, back):
        to, device = plane_device(offset)
        source = lax.rem(me + 2 * low - offset, 2 * low) if back else me
        return pltpu.make_async_remote_copy(
            src_ref=shares.at[me],
            dst_ref=shares.at[source],
            send_sem=tell_send.at[offset - 1],
            recv_sem=tell_recv.at[offset - 1],
            device_id=device,
            device_id_type=MESH,
        )

    for offset in range(1, 2 * low):
        tell_plane(offset, False).start()
    for offset in range(1, 2 * low):
        tell_plane(offset, True).wait_recv()
    whole = shares[0]
    for spot in range(1, 2 * low):
        whole = whole + shares[spot]
    total_out[0, 0] = whole[0, 0]

    for span in range(spans):
        peer_copy(span).wait_send()
    for b in range(blocks):
        river_copy(b).wait_send()
        for offset in range(1, low):
            plane_copy(b, offset).wait_send()
        for offset in range(1, high):
            line_copy(b, offset).wait_send()
    for offset in range(1, 2 * low):
        tell_plane(offset, False).wait_send()


def solution(mesh):
    n_node = mesh.shape["node"]
    high = min(4, n_node)
    low = n_node // high

    def local(
        ranges, strengths, live_hands, pot_sizes, action_counts, parents, turn_counts, root_reach
    ):
        nodes, line_rows, half = ranges.shape
        hands = strengths.shape[1]
        tiles = -(-half // WIDE) * 2
        blocks = tiles // 2
        turns_all = turn_counts.shape[0]
        turns_mine = turns_all // n_node
        rows_all = turns_all * 2 * TACT
        out_rows = turns_mine * 2 * TACT
        mine = nodes // 2
        spans = mine // TALL
        f32, bf16 = jnp.float32, jnp.bfloat16
        vmem = pl.BlockSpec(memory_space=pltpu.VMEM)
        smem = pl.BlockSpec(memory_space=pltpu.SMEM)
        hbm = pl.BlockSpec(memory_space=pl.ANY)
        dma = pltpu.SemaphoreType.DMA
        sizes = (n_node, low, high, nodes, half, tiles, turns_mine, rows_all)
        best, total = pl.pallas_call(
            functools.partial(kernel, sizes),
            out_shape=(
                jax.ShapeDtypeStruct((turns_mine, 2, half), f32),
                jax.ShapeDtypeStruct((1, 1), f32),
            ),
            in_specs=[hbm, vmem, vmem, vmem, smem, vmem, smem, vmem, hbm],
            out_specs=(vmem, smem),
            scratch_shapes=[
                pltpu.VMEM((2, spans, tiles * LANE, TALL, line_rows), bf16),
                [pltpu.VMEM((LANE * TALL, line_rows), f32) for _ in range(2)],
                pltpu.VMEM((mine, 2 * tiles, line_rows, LANE), bf16),
                pltpu.VMEM((2, tiles, mine, LANE), f32),
                pltpu.VMEM((2, tiles, mine, LANE), f32),
                pltpu.VMEM((mine, 2 * tiles * LANE, LANE), bf16),
                pltpu.VMEM((2 * tiles, 2 * tiles * LANE, LANE), jnp.int8),
                pltpu.VMEM((mine, line_rows, LANE), f32),
                [pltpu.VMEM((line_rows, LANE), f32) for _ in range(2 * TALL)],
                pltpu.VMEM((2, blocks, 2, 2, mine, LANE), f32),
                pltpu.VMEM((blocks, 2, 2, mine, LANE), f32),
                pltpu.VMEM((rows_all, 12 * mine), bf16),
                pltpu.VMEM((blocks, low, high, out_rows, WIDE), f32),
                pltpu.VMEM((blocks, low - 1, high, out_rows, WIDE), f32),
                pltpu.VMEM((blocks, high, high, out_rows, WIDE), f32),
                pltpu.VMEM((high, turns_mine, 2, half), f32),
                pltpu.VMEM((2 * low, 1, LANE), f32),
                dma,
                dma((spans,)),
                dma((spans,)),
                dma((spans,)),
                dma((blocks,)),
                dma((blocks,)),
                dma((blocks, low - 1)),
                dma((blocks, low - 1)),
                dma((blocks, high - 1)),
                dma((blocks, high - 1)),
                dma((2 * low - 1,)),
                dma((2 * low - 1,)),
            ],
            compiler_params=pltpu.CompilerParams(
                collective_id=0, has_side_effects=True, vmem_limit_bytes=60 * 1024 * 1024
            ),
        )(
            jnp.transpose(ranges, (2, 0, 1)),
            strengths,
            live_hands,
            pot_sizes,
            action_counts,
            parents.reshape(1, nodes),
            turn_counts,
            root_reach,
            compat_table(hands, half, tiles),
        )
        return best, total.reshape(())

    in_specs = (
        P("node", None, "hand"),
        P("node", None),
        P("node", None),
        P("node", None),
        P("node"),
        P("node"),
        P(),
        P(None, None, "hand"),
    )
    out_specs = (P("node", None, "hand"), P())
    return jax.shard_map(local, mesh=mesh, in_specs=in_specs, out_specs=out_specs, check_vma=False)
```
